256 devices in a mesh: rep: 2 (over core), dp: 128 (over x, y, z).
Axes of the slice: x: 4, y: 4, z: 8, core: 2. Of those that a mesh axis runs over, the one named last changes fastest.
Arguments:
- x: bfloat16 [256, 2048, 640], P(('rep', 'dp')), parts along dimension 0
- dy: bfloat16 [256, 2048, 640], P(('rep', 'dp')), parts along dimension 0
- w_gate: bfloat16 [2, 640, 3200], P(None, 'dp')
- w_up: bfloat16 [2, 640, 3200], P(None, 'dp')
- w_down: bfloat16 [2, 3200, 640], P(None, 'dp')
Outputs:
- output 1: bfloat16 [256, 2048, 640], P(('rep', 'dp')), parts along dimension 0
- output 2: bfloat16 [4, 640, 3200], P('rep', 'dp'), parts along dimension 0
- output 3: bfloat16 [4, 640, 3200], P('rep', 'dp'), parts along dimension 0
- output 4: bfloat16 [4, 3200, 640], P('rep', 'dp'), parts along dimension 0
There are 2 independent parts. The reference program is written for one: setup_inputs(seed, part) draws one part's arguments, and reference() takes and returns one part's arrays. A program takes and returns all parts, laid end to end along the dimension named above; an argument that names none is the same for every part.
All inputs are finite; a program needn't handle non-finite values.
Results may differ from the reference program's by a relative error of at most 0.018.
Values are sent between devices in bfloat16 or wider.
A program may use at most 768 MiB of HBM per device.

```python
import jax
import jax.numpy as jnp
from jax import lax

SEQUENCES = 128
TOKENS = 2048
D = 640
FF = 3200
LAYERS = 2
NAMES = ("w_gate", "w_up", "w_down")
SHAPES = {"w_gate": (LAYERS, D, FF), "w_up": (LAYERS, D, FF), "w_down": (LAYERS, FF, D)}


def bump(key, n, height):
    away = (jnp.arange(n, dtype=jnp.int32) - jax.random.randint(key, (), 0, n, jnp.int32)) % n
    return jnp.where(away < n // 8, height, 1.0)


def together(key, own, strength):
    shared = jax.random.normal(key, own.shape[1:], jnp.float32)
    return (own + strength * shared) * lax.rsqrt(1 + strength * strength)


def setup_inputs(seed: int = 0, part: int = 0) -> dict:
    kx, kdy, ka, kb, kz, kf, kh, kl, *kw = jax.random.split(jax.random.key(seed), 8 + len(NAMES))
    kx, kdy, ka, kb = (jax.random.fold_in(k, part) for k in (kx, kdy, ka, kb))
    shape = (SEQUENCES, TOKENS, D)
    much_x, much_dy = jax.random.uniform(kz, (2,), jnp.float32, 0.0, 1.0)
    layers = 2.0 ** jax.random.uniform(kl, (LAYERS, 1, 1), jnp.float32, -1.0, 1.0)
    x = together(ka, jax.random.normal(kx, shape, jnp.float32), much_x) * bump(kf, D, 4.0)
    dy = together(kb, jax.random.normal(kdy, shape, jnp.float32), much_dy)
    drawn = {"x": x.astype(jnp.bfloat16), "dy": (dy * (SEQUENCES * TOKENS) ** -0.5).astype(jnp.bfloat16)}
    for key, name in zip(kw, NAMES, strict=True):
        w = jax.random.normal(key, SHAPES[name], jnp.float32) * SHAPES[name][1] ** -0.5
        drawn[name] = (w * {"w_gate": 1.0, "w_up": bump(kh, FF, 4.0), "w_down": layers}[name]).astype(jnp.bfloat16)
    return drawn


def matmul(a, w):
    return jnp.dot(a, w, preferred_element_type=jnp.float32).astype(jnp.bfloat16)


def normed(h):
    wide = h.astype(jnp.float32)
    scale = lax.rsqrt(jnp.mean(wide**2, -1, keepdims=True) + 1e-6)
    return (wide * scale).astype(jnp.bfloat16)


def layer(h, w):
    a = normed(h)
    gate = jnp.dot(a, w["w_gate"], preferred_element_type=jnp.float32)
    up = jnp.dot(a, w["w_up"], preferred_element_type=jnp.float32)
    return h + matmul((jax.nn.silu(gate) * up).astype(jnp.bfloat16), w["w_down"])


def stack(weights, h):
    return lax.scan(lambda h, w: (layer(h, w), None), h, weights)[0]


def reference(x, dy, w_gate, w_up, w_down):
    weights = dict(zip(NAMES, (w_gate, w_up, w_down), strict=True))

    def take(so_far, sequence):
        h, by_y = sequence
        _, back = jax.vjp(stack, weights, h)
        by_weights, by_h = back(by_y)
        return jax.tree.map(lambda total, term: total + term.astype(jnp.float32), so_far, by_weights), by_h

    none_yet = {name: jnp.zeros(w.shape, jnp.float32) for name, w in weights.items()}
    by_weights, by_x = lax.scan(take, none_yet, (x, dy))
    return (by_x, *(by_weights[name].astype(jnp.bfloat16) for name in NAMES))
```

```python
import jax
import jax.numpy as jnp
from jax import lax
from jax.sharding import Mesh, PartitionSpec as P

F32, BF16 = jnp.float32, jnp.bfloat16


def dot(a, b, ca, cb):
    return lax.dot_general(a, b, (((ca,), (cb,)), ((), ())), preferred_element_type=F32)


def norm_parts(h):
    wide = h.astype(F32)
    scale = lax.rsqrt(jnp.mean(wide**2, -1, keepdims=True) + 1e-6)
    return wide, scale


def forward(h, wg, wu, wd, last):
    wide, scale = norm_parts(h)
    a = (wide * scale).astype(BF16)
    gate, up = dot(a, wg, 1, 0), dot(a, wu, 1, 0)
    p = (jax.nn.silu(gate) * up).astype(BF16)
    out = None if last else h + dot(p, wd, 1, 0).astype(BF16)
    return out, (wide, scale, a, gate, up, p)


def backward(d, saved, wg, wu, wd):
    wide, scale, a, gate, up, p = saved
    dp = dot(d, wd, 1, 1).astype(BF16).astype(F32)
    dwd = dot(p, d, 0, 0).astype(BF16)
    sig = jax.nn.sigmoid(gate)
    dg = (dp * up * (sig * (1 + gate * (1 - sig)))).astype(BF16)
    du = (dp * gate * sig).astype(BF16)
    dwg, dwu = dot(a, dg, 0, 0).astype(BF16), dot(a, du, 0, 0).astype(BF16)
    da = (dot(dg, wg, 1, 1).astype(BF16) + dot(du, wu, 1, 1).astype(BF16)).astype(F32)
    inner = jnp.sum(da * wide, -1, keepdims=True) / wide.shape[-1]
    dwide = da * scale - wide * (scale**3 * inner)
    return d + dwide.astype(BF16), dwg, dwu, dwd


def solution(mesh):
    groups, n = mesh.shape["rep"], mesh.shape["dp"]
    fine = Mesh(mesh.devices.reshape(groups, 4, 4, n // 16), ("rep", "x", "y", "z"))
    every = ("x", "y", "z")

    def step(x, dy, wg, wu, wd):
        d_model, ff = wg.shape[1] * n, wg.shape[2]
        wg0 = lax.all_gather(wg[0], every, axis=0, tiled=True)
        wu0 = lax.all_gather(wu[0].reshape(-1, 128), every, axis=0, tiled=True).reshape(d_model, ff)
        wd0 = wd[0]
        for axis in ("z", "y", "x"):
            wd0 = lax.all_gather(wd0, axis, axis=0, tiled=True)
        flat = jnp.concatenate([t[1].reshape(-1, 128) for t in (wg, wu, wd)])
        flat = lax.all_gather(flat, every, axis=0)
        cuts = (0, wg[1].size // 128, 2 * wg[1].size // 128, flat.shape[1])
        wg1, wu1, wd1 = (flat[:, lo:hi].reshape(s) for lo, hi, s in zip(cuts[:-1], cuts[1:], ((d_model, ff), (d_model, ff), (ff, d_model))))

        h0, dh = x[0], dy[0]
        h1, saved0 = forward(h0, wg0, wu0, wd0, False)
        _, saved1 = forward(h1, wg1, wu1, wd1, True)
        dh, g1, u1, d1 = backward(dh, saved1, wg1, wu1, wd1)
        flat = jnp.concatenate([t.reshape(n, -1, 128) for t in (g1, u1, d1)], 1)
        flat = flat.reshape(4, 4, -1, *flat.shape[1:])
        for axis in every:
            flat = lax.psum_scatter(flat, axis, scatter_dimension=0)
        g1, u1, d1 = (flat[lo:hi].reshape(s) for lo, hi, s in zip(cuts[:-1], cuts[1:], (wg.shape[1:], wu.shape[1:], wd.shape[1:])))
        dh, g0, u0, d0 = backward(dh, saved0, wg0, wu0, wd0)
        for axis in every:
            d0 = lax.psum_scatter(d0, axis, scatter_dimension=0, tiled=True)
        u0 = u0.reshape(16, -1, 128)
        u0 = lax.psum_scatter(u0, ("x", "y"), scatter_dimension=0)
        u0 = lax.psum_scatter(u0, "z", scatter_dimension=0, tiled=True).reshape(wu.shape[1:])
        for axis in ("x", "y", "z"):
            g0 = lax.psum_scatter(g0, axis, scatter_dimension=0, tiled=True)
        return dh[None], jnp.stack([g0, g1]), jnp.stack([u0, u1]), jnp.stack([d0, d1])

    data = P(("rep", *every), None, None)
    weight = P(None, every, None)
    grad = P("rep", every, None)
    return jax.shard_map(step, mesh=fine, in_specs=(data, data, weight, weight, weight), out_specs=(data, grad, grad, grad), check_vma=False)
```

```python
import functools

import jax
import jax.numpy as jnp
from jax import lax
from jax.experimental import pallas as pl
from jax.experimental.pallas import tpu as pltpu
from jax.sharding import PartitionSpec as P

F32, BF16 = jnp.float32, jnp.bfloat16
MESH = pl.DeviceIdType.MESH
SIDE = 4
VMEM = pltpu.VMEM
DMA = pltpu.SemaphoreType.DMA


def place(depth):
    me = lax.axis_index("dp")
    z = lax.rem(me, depth)
    y = lax.rem(me // depth, SIDE)
    x = me // (depth * SIDE)
    return lax.axis_index("rep"), x, y, z, lambda x, y, z: (x * SIDE + y) * depth + z


def turn(i, by, n):
    return lax.rem(i + by + n, n)


def meet(peers):
    barrier = pltpu.get_barrier_semaphore()
    for peer in peers:
        pl.semaphore_signal(barrier, inc=1, device_id=peer, device_id_type=MESH)
    pl.semaphore_wait(barrier, len(peers))


class Copies:
    def __init__(self, send, recv):
        self.send, self.recv, self.used, self.open = send, recv, 0, []

    def make(self, src, dst, peer):
        k = self.used
        self.used += 1
        return pltpu.make_async_remote_copy(src, dst, self.send.at[k], self.recv.at[k], device_id=peer, device_id_type=MESH)

    def start(self, src, dst, peer):
        copy = self.make(src, dst, peer)
        copy.start()
        self.open.append(copy)
        return copy

    def drain(self):
        for copy in self.open:
            copy.wait_send()
        self.open = []


def z_gather_kernel(depth, parts, own, out, send, recv, local):
    core, x, y, z, index = place(depth)
    right, left = ({"dp": index(x, y, turn(z, by, depth))} for by in (1, -1))
    partner = {"rep": 1 - core}
    half = parts // 2
    fill = pltpu.make_async_copy(own, out.at[z], local)
    fill.start()
    meet((right, left, partner))
    copies = Copies(send, recv)

    def block(by, j):
        return out.at[turn(z, by, depth), core * half + j]

    fill.wait()
    from_left, from_right, relays = {}, {}, []
    steps = depth // 2
    for s in range(steps + 1):
        for j in range(half):
            if s:
                from_left[s - 1, j].wait_recv()
                relays.append(copies.start(block(-s, j), block(-s, j), partner))
            if s < steps:
                from_left[s, j] = copies.start(block(-s, j), block(-s, j), right)
            if 0 < s < depth - steps:
                from_right[s - 1, j].wait_recv()
                relays.append(copies.start(block(s, j), block(s, j), partner))
            if s < depth - 1 - steps:
                from_right[s, j] = copies.start(block(s, j), block(s, j), left)
    for relay in relays:
        relay.wait_recv()
    copies.drain()


def z_gather(own, depth, cid):
    parts = own.shape[0]
    count = parts // 2 * (depth - 1) * 2
    return pl.pallas_call(
        functools.partial(z_gather_kernel, depth, parts),
        out_shape=jax.ShapeDtypeStruct((depth, *own.shape), own.dtype),
        in_specs=[pl.BlockSpec(memory_space=pl.ANY)],
        out_specs=pl.BlockSpec(memory_space=VMEM),
        scratch_shapes=[DMA((count,)), DMA((count,)), DMA],
        compiler_params=pltpu.CompilerParams(collective_id=cid, has_side_effects=True),
        name="z_gather",
    )(own)


def columns(n):
    cut = -(-n // 256) * 128
    return pl.ds(0, cut), pl.ds(cut, n - cut)


def cut_rows(ref):
    lead = ref.shape[0]
    cut = 2 if len(ref.shape) == 3 else -(-lead // 16) * 8
    return ref.at[pl.ds(0, cut)], ref.at[pl.ds(cut, lead - cut)]


def gather_half(copies, region, pos, right, left, partner):
    own, before, after, far = (region(turn(pos, by, SIDE)) for by in (0, -1, 1, 2))
    to_right = copies.start(own, own, right)
    to_left = copies.start(own, own, left)
    yield
    to_right.wait_recv()
    first, second = cut_rows(before)[0], cut_rows(after)[1]
    go = copies.start(first, first, right)
    to_left.wait_recv()
    back = copies.start(second, second, left)
    relays = [copies.start(before, before, partner), copies.start(after, after, partner)]
    yield
    go.wait_recv()
    back.wait_recv()
    relays.append(copies.start(far, far, partner))
    return relays


def gather_job(copies, ref, core_ring, which):
    x, y, xr, xl, yr, yl, partner = core_ring
    cols = columns(ref.shape[-1])[which]
    one = lambda i, j: ref.at[i, j, :, cols]
    if which == 0:
        relays = yield from gather_half(copies, lambda i: one(x, i), y, yr, yl, partner)
        relays += yield from gather_half(copies, lambda i: ref.at[i, :, :, cols], x, xr, xl, partner)
    else:
        relays = yield from gather_half(copies, lambda i: one(i, y), x, xr, xl, partner)
        relays += yield from gather_half(copies, lambda i: ref.at[:, i, :, cols], y, yr, yl, partner)
    return relays


GATHER_COPIES = 2 * (4 + 3)


def neighbours(depth):
    core, x, y, z, index = place(depth)
    xr, xl = ({"dp": index(turn(x, by, SIDE), y, z)} for by in (1, -1))
    yr, yl = ({"dp": index(x, turn(y, by, SIDE), z)} for by in (1, -1))
    return core, (x, y, xr, xl, yr, yl, {"rep": 1 - core})


def run_together(jobs):
    done = [None] * len(jobs)
    live = list(range(len(jobs)))
    while live:
        for k in list(live):
            try:
                next(jobs[k])
            except StopIteration as stop:
                done[k] = stop.value
                live.remove(k)
    return done


def xy_gather_kernel(depth, own0, own1, own2, out0, out1, out2, send, recv, local):
    core, ring = neighbours(depth)
    x, y = ring[:2]
    fills = []
    for own, out in ((own0, out0), (own1, out1), (own2, out2)):
        for k in range(2):
            fills.append(pltpu.make_async_copy(own.at[k], out.at[k, x, y], local.at[len(fills)]))
            fills[-1].start()
    meet(ring[2:])
    for fill in fills:
        fill.wait()
    copies = Copies(send, recv)
    jobs = [gather_job(copies, out.at[core], ring, which) for out in (out0, out2, out1) for which in range(2)]
    for relays in run_together(jobs):
        for relay in relays:
            relay.wait_recv()
    copies.drain()


def xy_gather(own0, own1, own2, depth, cid):
    owns = (own0, own1, own2)
    count = 6 * GATHER_COPIES
    return pl.pallas_call(
        functools.partial(xy_gather_kernel, depth),
        out_shape=[jax.ShapeDtypeStruct((2, SIDE, SIDE, *own.shape[1:]), own.dtype) for own in owns],
        in_specs=[pl.BlockSpec(memory_space=pl.ANY)] * 3,
        out_specs=[pl.BlockSpec(memory_space=pl.ANY)] * 3,
        scratch_shapes=[DMA((count,)), DMA((count,)), DMA((6,))],
        compiler_params=pltpu.CompilerParams(collective_id=cid, has_side_effects=True),
        name="xy_gather",
    )(*owns)


def each_block(fn, lead):
    if lead is None:
        fn(())
    else:
        pl.loop(0, lead)(lambda i: fn((i,)))


def add_up(dst, parts):
    lead = dst.shape[0] if len(dst.shape) == 3 else None

    def block(at):
        total = parts[0][at].astype(F32) if at else parts[0][...].astype(F32)
        for part in parts[1:]:
            total += (part[at] if at else part[...]).astype(F32)
        if at:
            dst[at] = total.astype(dst.dtype)
        else:
            dst[...] = total.astype(dst.dtype)

    each_block(block, lead)


def scatter_half(copies, term, exact, buffers, pos, right, left, dst):
    far_l, far_r, near_l, near_r, out_l, out_r = buffers
    ahead, behind = turn(pos, 1, SIDE), turn(pos, -1, SIDE)
    far0, far1 = cut_rows(term(turn(pos, 2, SIDE)))
    after0, before1 = cut_rows(term(ahead))[0], cut_rows(term(behind))[1]
    (nl0, nl1), (nr0, nr1) = map(cut_rows, (near_l, near_r))
    to_left = copies.start(far0, far_r, left)
    to_right = copies.start(far1, far_l, right)
    plain = [copies.start(after0, nl0, right), copies.start(before1, nr1, left)]
    yield
    to_left.wait_recv()
    add_up(out_l, (cut_rows(exact(behind))[0], far_r))
    plain.append(copies.start(out_l, nr0, left))
    to_right.wait_recv()
    add_up(out_r, (cut_rows(exact(ahead))[1], far_l))
    plain.append(copies.start(out_r, nl1, right))
    yield
    for copy in plain:
        copy.wait_recv()
    add_up(dst, (exact(pos), near_l, near_r))


SCATTER_COPIES = 2 * 6


def scatter_job(copies, ref, order, ring, first, total, cast, second, out):
    x, y, xr, xl, yr, yl = ring
    along_x, along_y = (x, xr, xl), (y, yr, yl)
    if order == 0:
        one, two, term = along_x, along_y, lambda i: ref.at[i]
    else:
        one, two, term = along_y, along_x, lambda i: ref.at[:, i]
    yield from scatter_half(copies, term, term, first, *one, total)

    @pl.loop(0, SIDE)
    def _(i):
        cast[i] = total[i].astype(BF16)

    yield from scatter_half(copies, lambda i: cast.at[i], lambda i: total.at[i], second, *two, out)


def scatter_scratch(rows, cols):
    cut = -(-rows // 16) * 8
    half, whole = VMEM((2, rows, cols), BF16), VMEM((SIDE, rows, cols), BF16)
    near, top, low = VMEM((rows, cols), BF16), VMEM((cut, cols), BF16), VMEM((rows - cut, cols), BF16)
    first = [half, half, whole, whole, half, half]
    second = [low, top, near, near, top, low]
    return [*first, VMEM((SIDE, rows, cols), F32), whole, *second]


def xy_scatter_kernel(depth, *refs):
    ins, outs, (send, recv), scratch = refs[:3], refs[3:6], refs[6:8], refs[8:]
    _, ring = neighbours(depth)
    meet(ring[2:-1])
    copies = Copies(send, recv)
    jobs = []
    for ref, out in zip(ins, outs):
        for which in range(2):
            mine, scratch = scratch[:14], scratch[14:]
            cols = columns(ref.shape[-1])[which]
            jobs.append(scatter_job(copies, ref.at[:, :, :, cols], which, ring[:-1], mine[:6], mine[6], mine[7], mine[8:], out.at[:, cols]))
    run_together(jobs)
    copies.drain()


def xy_scatter(terms, depth, cid):
    scratch = [DMA((6 * SCATTER_COPIES,)), DMA((6 * SCATTER_COPIES,))]
    for term in terms:
        scratch += [spec for cols in columns(term.shape[-1]) for spec in scatter_scratch(term.shape[2], cols.size)]
    return pl.pallas_call(
        functools.partial(xy_scatter_kernel, depth),
        out_shape=[jax.ShapeDtypeStruct(term.shape[2:], F32) for term in terms],
        in_specs=[pl.BlockSpec(memory_space=VMEM)] * 3,
        out_specs=[pl.BlockSpec(memory_space=VMEM)] * 3,
        scratch_shapes=scratch,
        compiler_params=pltpu.CompilerParams(collective_id=cid, has_side_effects=True, vmem_limit_bytes=60 << 20),
        name="xy_scatter",
    )(*terms)


def z_scatter_kernel(depth, parts, own, out, in_r, out_r, in_l, out_l, send, recv):
    _, x, y, z, index = place(depth)
    right, left = ({"dp": index(x, y, turn(z, by, depth))} for by in (1, -1))
    meet((right, left))
    copies = Copies(send, recv)
    n_right = depth // 2
    n_left = depth - 1 - n_right
    going = {}
    for s in range(n_right):
        for j in range(parts):
            for way, steps, inbox, outbox, peer in ((1, n_right, in_r, out_r, right), (-1, n_left, in_l, out_l, left)):
                if s >= steps:
                    continue
                value = own[turn(z, way * (steps - s), depth), j]
                if s:
                    going[way, s - 1, j].wait_recv()
                    value += inbox[s - 1, j].astype(F32)
                outbox[s, j] = value.astype(BF16)
                going[way, s, j] = copies.start(outbox.at[s, j], inbox.at[s, j], peer)
    for j in range(parts):
        value = own[z, j]
        for way, steps, inbox in ((1, n_right, in_r), (-1, n_left, in_l)):
            if steps:
                going[way, steps - 1, j].wait_recv()
                value += inbox[steps - 1, j].astype(F32)
        out[j] = value.astype(BF16)
    copies.drain()


def z_scatter(own, cid):
    depth, parts, rows, lanes = own.shape
    boxes = [VMEM((max(steps, 1), parts, rows, lanes), BF16) for steps in (depth // 2, depth // 2, depth - 1 - depth // 2, depth - 1 - depth // 2)]
    count = parts * (depth - 1)
    return pl.pallas_call(
        functools.partial(z_scatter_kernel, depth, parts),
        out_shape=jax.ShapeDtypeStruct(own.shape[1:], BF16),
        in_specs=[pl.BlockSpec(memory_space=VMEM)],
        out_specs=pl.BlockSpec(memory_space=VMEM),
        scratch_shapes=[*boxes, DMA((count,)), DMA((count,))],
        compiler_params=pltpu.CompilerParams(collective_id=cid, has_side_effects=True),
        name="z_scatter",
    )(own)


def flat(t):
    t = t.reshape(-1, 128)
    return jnp.pad(t, ((0, -t.shape[0] % 8), (0, 0)))


def unflat(t, shape):
    size = 1
    for n in shape:
        size *= n
    return t[..., : size // 128, :].reshape(*t.shape[:-2], *shape)


def gather_weights(wg, wu, wd, depth):
    own = jnp.stack([flat(t) for t in (wg[0], wg[1], wd[0], wu[0], wu[1], wd[1])])
    got = z_gather(own, depth, 1)
    g0, g1, d0, u0, u1, d1 = (unflat(got[:, k], t.shape[1:]).reshape(-1, t.shape[2]) for k, t in enumerate((wg, wg, wd, wu, wu, wd)))
    return xy_gather(jnp.stack([g0, u0]), jnp.stack([g1, u1]), jnp.stack([d0, d1]), depth, 2)


def scatter_grads(sums, shapes, depth):
    own = []
    for t, shape in zip(sums, shapes):
        t = t.reshape(depth, -1, 128)
        own.append(jnp.pad(t, ((0, 0), (0, -t.shape[1] % 8), (0, 0))))
    out = z_scatter(jnp.stack(own, 1), 5)
    return [unflat(out[k], shape) for k, shape in enumerate(shapes)]


def dot(a, b, ca, cb):
    return lax.dot_general(a, b, (((ca,), (cb,)), ((), ())), preferred_element_type=F32)


def norm_parts(h):
    wide = h.astype(F32)
    scale = lax.rsqrt(jnp.mean(wide**2, -1, keepdims=True) + 1e-6)
    return wide, scale


def forward(h, wg, wu, wd, last):
    wide, scale = norm_parts(h)
    a = (wide * scale).astype(BF16)
    gate, up = dot(a, wg, 1, 0), dot(a, wu, 1, 0)
    p = (jax.nn.silu(gate) * up).astype(BF16)
    out = None if last else h + dot(p, wd, 1, 0).astype(BF16)
    return out, (wide, scale, a, gate, up, p)


def backward(d, saved, wg, wu, wd):
    wide, scale, a, gate, up, p = saved
    dp = dot(d, wd, 1, 1).astype(BF16).astype(F32)
    dwd = dot(p, d, 0, 0).astype(BF16)
    sig = jax.nn.sigmoid(gate)
    dg = (dp * up * (sig * (1 + gate * (1 - sig)))).astype(BF16)
    du = (dp * gate * sig).astype(BF16)
    dwg, dwu = dot(a, dg, 0, 0).astype(BF16), dot(a, du, 0, 0).astype(BF16)
    da = (dot(dg, wg, 1, 1).astype(BF16) + dot(du, wu, 1, 1).astype(BF16)).astype(F32)
    inner = jnp.sum(da * wide, -1, keepdims=True) / wide.shape[-1]
    dwide = da * scale - wide * (scale**3 * inner)
    return d + dwide.astype(BF16), dwg, dwu, dwd


def solution(mesh):
    n = mesh.shape["dp"]
    depth = n // SIDE**2

    def step(x, dy, wg, wu, wd):
        d_model, ff = wg.shape[1] * n, wg.shape[2]
        gu0, gu1, down = gather_weights(wg, wu, wd, depth)
        wg0, wu0, wg1, wu1 = (t.reshape(d_model, ff) for t in (*gu0, *gu1))
        wd0, wd1 = (t.reshape(ff, d_model) for t in down)
        h1, saved0 = forward(x[0], wg0, wu0, wd0, False)
        _, saved1 = forward(h1, wg1, wu1, wd1, True)
        dh, *terms1 = backward(dy[0], saved1, wg1, wu1, wd1)
        dh, *terms0 = backward(dh, saved0, wg0, wu0, wd0)
        sums = []
        for k, terms in enumerate((terms0, terms1)):
            sums += xy_scatter([t.reshape(SIDE, SIDE, -1, t.shape[1]) for t in terms], depth, 3 + k)
        g0, u0, d0, g1, u1, d1 = scatter_grads(sums, [t.shape[1:] for t in (wg, wu, wd)] * 2, depth)
        return dh[None], jnp.stack([g0, g1]), jnp.stack([u0, u1]), jnp.stack([d0, d1])

    data = P(("rep", "dp"), None, None)
    weight = P(None, "dp", None)
    grad = P("rep", "dp", None)
    return jax.shard_map(step, mesh=mesh, in_specs=(data, data, weight, weight, weight), out_specs=(data, grad, grad, grad), check_vma=False)
```

```python
import functools

import jax
import jax.numpy as jnp
from jax import lax
from jax.experimental import pallas as pl
from jax.experimental.pallas import tpu as pltpu
from jax.sharding import PartitionSpec as P

F32, BF16 = jnp.float32, jnp.bfloat16
MESH = pl.DeviceIdType.MESH
SIDE = 4
VMEM = pltpu.VMEM
DMA = pltpu.SemaphoreType.DMA


def place(depth):
    me = lax.axis_index("dp")
    z = lax.rem(me, depth)
    y = lax.rem(me // depth, SIDE)
    x = me // (depth * SIDE)
    return lax.axis_index("rep"), x, y, z, lambda x, y, z: (x * SIDE + y) * depth + z


def turn(i, by, n):
    return lax.rem(i + by + n, n)


def meet(peers):
    barrier = pltpu.get_barrier_semaphore()
    for peer in peers:
        pl.semaphore_signal(barrier, inc=1, device_id=peer, device_id_type=MESH)
    pl.semaphore_wait(barrier, len(peers))


class Copies:
    def __init__(self, send, recv):
        self.send, self.recv, self.used, self.open = send, recv, 0, []

    def make(self, src, dst, peer):
        k = self.used
        self.used += 1
        return pltpu.make_async_remote_copy(src, dst, self.send.at[k], self.recv.at[k], device_id=peer, device_id_type=MESH)

    def start(self, src, dst, peer):
        copy = self.make(src, dst, peer)
        copy.start()
        self.open.append(copy)
        return copy

    def drain(self):
        for copy in self.open:
            copy.wait_send()
        self.open = []


def z_gather_kernel(depth, parts, own, out, send, recv, local):
    core, x, y, z, index = place(depth)
    right, left = ({"dp": index(x, y, turn(z, by, depth))} for by in (1, -1))
    partner = {"rep": 1 - core}
    half = parts // 2
    fill = pltpu.make_async_copy(own, out.at[z], local)
    fill.start()
    meet((right, left, partner))
    copies = Copies(send, recv)

    def block(by, j):
        return out.at[turn(z, by, depth), core * half + j]

    fill.wait()
    from_left, from_right, relays = {}, {}, []
    steps = depth // 2
    for s in range(steps + 1):
        for j in range(half):
            if s:
                from_left[s - 1, j].wait_recv()
                relays.append(copies.start(block(-s, j), block(-s, j), partner))
            if s < steps:
                from_left[s, j] = copies.start(block(-s, j), block(-s, j), right)
            if 0 < s < depth - steps:
                from_right[s - 1, j].wait_recv()
                relays.append(copies.start(block(s, j), block(s, j), partner))
            if s < depth - 1 - steps:
                from_right[s, j] = copies.start(block(s, j), block(s, j), left)
    for relay in relays:
        relay.wait_recv()
    copies.drain()


def z_gather(own, depth, cid):
    parts = own.shape[0]
    count = parts // 2 * (depth - 1) * 2
    return pl.pallas_call(
        functools.partial(z_gather_kernel, depth, parts),
        out_shape=jax.ShapeDtypeStruct((depth, *own.shape), own.dtype),
        in_specs=[pl.BlockSpec(memory_space=pl.ANY)],
        out_specs=pl.BlockSpec(memory_space=VMEM),
        scratch_shapes=[DMA((count,)), DMA((count,)), DMA],
        compiler_params=pltpu.CompilerParams(collective_id=cid, has_side_effects=True),
        name="z_gather",
    )(own)


def columns(n):
    cut = -(-n // 256) * 128
    return pl.ds(0, cut), pl.ds(cut, n - cut)


def cut_rows(ref):
    lead = ref.shape[0]
    cut = -(-lead // 2) if len(ref.shape) > 2 else -(-lead // 16) * 8
    return ref.at[pl.ds(0, cut)], ref.at[pl.ds(cut, lead - cut)]


def gather_half(copies, region, pos, right, left, partner):
    own, before, after, far = (region(turn(pos, by, SIDE)) for by in (0, -1, 1, 2))
    to_right = copies.start(own, own, right)
    to_left = copies.start(own, own, left)
    yield
    to_right.wait_recv()
    first, second = cut_rows(before)[0], cut_rows(after)[1]
    go = copies.start(first, first, right)
    to_left.wait_recv()
    back = copies.start(second, second, left)
    relays = [copies.start(before, before, partner), copies.start(after, after, partner)]
    yield
    go.wait_recv()
    back.wait_recv()
    relays.append(copies.start(far, far, partner))
    return relays


def gather_job(copies, ref, core_ring, which):
    x, y, xr, xl, yr, yl, partner = core_ring
    cols = columns(ref.shape[-1])[which]
    one = lambda i, j: ref.at[i, j, :, cols]
    if which == 0:
        relays = yield from gather_half(copies, lambda i: one(x, i), y, yr, yl, partner)
        relays += yield from gather_half(copies, lambda i: ref.at[i, :, :, cols], x, xr, xl, partner)
    else:
        relays = yield from gather_half(copies, lambda i: one(i, y), x, xr, xl, partner)
        relays += yield from gather_half(copies, lambda i: ref.at[:, i, :, cols], y, yr, yl, partner)
    return relays


GATHER_COPIES = 2 * (4 + 3)


def neighbours(depth):
    core, x, y, z, index = place(depth)
    xr, xl = ({"dp": index(turn(x, by, SIDE), y, z)} for by in (1, -1))
    yr, yl = ({"dp": index(x, turn(y, by, SIDE), z)} for by in (1, -1))
    return core, (x, y, xr, xl, yr, yl, {"rep": 1 - core})


def run_together(jobs):
    done = [None] * len(jobs)
    live = list(range(len(jobs)))
    while live:
        for k in list(live):
            try:
                next(jobs[k])
            except StopIteration as stop:
                done[k] = stop.value
                live.remove(k)
    return done


def xy_gather_kernel(depth, own0, own1, own2, out0, out1, out2, send, recv, local):
    core, ring = neighbours(depth)
    x, y = ring[:2]
    fills = []
    for own, out in ((own0, out0), (own1, out1), (own2, out2)):
        for k in range(2):
            fills.append(pltpu.make_async_copy(own.at[k], out.at[k, x, y], local.at[len(fills)]))
            fills[-1].start()
    meet(ring[2:])
    for fill in fills:
        fill.wait()
    copies = Copies(send, recv)
    jobs = [gather_job(copies, out.at[core], ring, which) for out in (out0, out2, out1) for which in range(2)]
    for relays in run_together(jobs):
        for relay in relays:
            relay.wait_recv()
    copies.drain()


def xy_gather(own0, own1, own2, depth, cid):
    owns = (own0, own1, own2)
    count = 6 * GATHER_COPIES
    return pl.pallas_call(
        functools.partial(xy_gather_kernel, depth),
        out_shape=[jax.ShapeDtypeStruct((2, SIDE, SIDE, *own.shape[1:]), own.dtype) for own in owns],
        in_specs=[pl.BlockSpec(memory_space=pl.ANY)] * 3,
        out_specs=[pl.BlockSpec(memory_space=pl.ANY)] * 3,
        scratch_shapes=[DMA((count,)), DMA((count,)), DMA((6,))],
        compiler_params=pltpu.CompilerParams(collective_id=cid, has_side_effects=True),
        name="xy_gather",
    )(*owns)


def add_up(dst, parts):
    lead = dst.shape[:-2]

    def block(at):
        total = parts[0][at].astype(F32)
        for part in parts[1:]:
            total += part[at].astype(F32)
        dst[at] = total.astype(dst.dtype)

    if not lead:
        block(...)
    elif len(lead) == 1:
        pl.loop(0, lead[0])(lambda i: block(i))
    else:
        pl.loop(0, lead[0])(lambda i: [block((i, j)) for j in range(lead[1])] and None)


def scatter_phase(send, recv, term, exact, buffers, pos, right, left, finish):
    far_l, far_r, near_l, near_r, out_l, out_r = buffers
    ahead, behind = turn(pos, 1, SIDE), turn(pos, -1, SIDE)
    far0, far1 = cut_rows(term(turn(pos, 2, SIDE)))
    after0, before1 = cut_rows(term(ahead))[0], cut_rows(term(behind))[1]
    before0, after1, own = cut_rows(exact(behind))[0], cut_rows(exact(ahead))[1], exact(pos)
    (nl0, nl1), (nr0, nr1) = map(cut_rows, (near_l, near_r))
    pairs = ((far0, far_r, left), (far1, far_l, right), (after0, nl0, right), (before1, nr1, left), (out_l, nr0, left), (out_r, nl1, right))
    copies = [
        pltpu.make_async_remote_copy(src, dst, send(k), recv(k), device_id=peer, device_id_type=MESH) for k, (src, dst, peer) in enumerate(pairs)
    ]

    def first():
        for copy in copies[:4]:
            copy.start()

    def second():
        copies[0].wait_recv()
        add_up(out_l, (before0, far_r))
        copies[4].start()
        copies[1].wait_recv()
        add_up(out_r, (after1, far_l))
        copies[5].start()

    def third():
        for copy in copies[2:]:
            copy.wait_recv()
        finish((own, near_l, near_r))
        for copy in copies:
            copy.wait_send()

    return first, second, third


def unit_scratch(rows, cols):
    whole = (SIDE, *rows, cols)
    half = (SIDE // 2, *rows, cols)
    cut = -(-rows[0] // 2) if len(rows) > 1 else -(-rows[0] // 16) * 8
    top, low = (cut, *rows[1:], cols), (rows[0] - cut, *rows[1:], cols)
    two = lambda shape: VMEM((2, *shape), BF16)
    near = (*rows, cols)
    first = [two(half), two(half), two(whole), two(whole), VMEM(half, BF16), VMEM(half, BF16)]
    second = [two(low), two(top), two(near), two(near), VMEM(top, BF16), VMEM(low, BF16)]
    return [*first, *second, VMEM((2, *whole), F32), two(whole)]


def unit_phases(kind, order, ring, sems, scratch, term, slot1, slot2, out):
    x, y, xr, xl, yr, yl = ring
    rings = ((x, xr, xl), (y, yr, yl))
    one, two = rings[order], rings[1 - order]
    region = (lambda i: term.at[i]) if order == 0 else (lambda i: term.at[:, i])
    total, cast = scratch[12:]
    send, recv = sems

    def buffers(k, slot):
        return [ref.at[slot] for ref in scratch[k : k + 4]] + list(scratch[k + 4 : k + 6])

    def keep(parts):
        add_up(total.at[slot1], parts)
        add_up(cast.at[slot1], (total.at[slot1],))

    def give(parts):
        add_up(out, parts)

    sem = lambda which, phase, slot: lambda k: which.at[kind, phase, slot, k]
    phase1 = scatter_phase(sem(send, 0, slot1), sem(recv, 0, slot1), region, region, buffers(0, slot1), *one, keep)
    phase2 = scatter_phase(
        sem(send, 1, slot2), sem(recv, 1, slot2), lambda i: cast.at[slot2, i], lambda i: total.at[slot2, i], buffers(6, slot2), *two, give
    )
    return phase1, phase2


CHUNK, TILE = 640, 512


def dot(a, b, ca=1, cb=0):
    return lax.dot_general(a, b, (((ca,), (cb,)), ((), ())), preferred_element_type=F32)


def scale_of(wide):
    return lax.rsqrt(jnp.mean(wide**2, -1, keepdims=True) + 1e-6)


def backward_kernel(depth, h0, h1, dy, p0, gu0, gu1, down, dx, sum_gu, sum_d, *scratch):
    (h, a, a_t, d, d_t, da, p, dg, du, w, gu_terms, d_terms), scratch = scratch[:12], scratch[12:]
    (load, load_w, send, recv), units = scratch[:4], scratch[4:]
    gu_units, d_units = (units[:14], units[14:28]), (units[28:42], units[42:])
    tokens, width = h.shape
    chunks = gu0.shape[2] // CHUNK
    blocks = d_terms.shape[3]
    rows = d_terms.shape[4]
    _, ring = neighbours(depth)
    ring = ring[:-1]
    meet(ring[2:])

    def weights(gu, layer, c, slot):
        cols = pl.ds(pl.multiple_of(c * CHUNK, CHUNK), CHUNK)
        sources = (gu.at[0, :, cols], gu.at[1, :, cols], down.at[layer, cols, :])
        return [pltpu.make_async_copy(src, w.at[slot, k], load_w.at[slot, k]) for k, src in enumerate(sources)]

    def prepare(h_hbm, d_hbm):
        copies = [pltpu.make_async_copy(h_hbm, h, load.at[0])]
        if d_hbm is not None:
            copies.append(pltpu.make_async_copy(d_hbm, d, load.at[1]))
        for copy in copies:
            copy.start()
        for copy in copies:
            copy.wait()

        @pl.loop(0, tokens // 256)
        def _(t):
            at = pl.ds(pl.multiple_of(t * 256, 256), 256)
            wide = h[at].astype(F32)
            normed = (wide * scale_of(wide)).astype(BF16)
            a[at] = normed
            a_t[:, at] = normed.T
            d_t[:, at] = d[at].T
            da[at] = jnp.zeros((256, width), F32)

    def finish():
        @pl.loop(0, tokens // 256)
        def _(t):
            at = pl.ds(pl.multiple_of(t * 256, 256), 256)
            wide = h[at].astype(F32)
            scale = scale_of(wide)
            by_a = da[at].astype(BF16).astype(F32)
            inner = jnp.mean(by_a * wide, -1, keepdims=True)
            by_h = (by_a * scale - wide * (scale * scale * scale * inner)).astype(BF16)
            d[at] = (d[at].astype(F32) + by_h.astype(F32)).astype(BF16)

    def down_term(layer, c):
        term = dot(d_t[...], p[...]).T
        for m in range(CHUNK // rows):
            g = c * (CHUNK // rows) + m
            d_terms[layer, g // (blocks * SIDE), lax.rem(g // blocks, SIDE), lax.rem(g, blocks)] = term[m * rows : (m + 1) * rows].astype(BF16)

    def tile(t, slot):
        at = pl.ds(pl.multiple_of(t * TILE, TILE), TILE)
        a_here = a[at]
        gate, up = dot(a_here, w[slot, 0]), dot(a_here, w[slot, 1])
        by_p = dot(d[at], w[slot, 2], 1, 1).astype(BF16).astype(F32)
        sig = jax.nn.sigmoid(gate)
        act = gate * sig
        p[at] = (act * up).astype(BF16)
        by_gate = (by_p * up * (sig + act * (1 - sig))).astype(BF16)
        by_up = (by_p * act).astype(BF16)
        dg[at] = by_gate
        du[at] = by_up
        da[at] += dot(by_gate, w[slot, 0], 1, 1) + dot(by_up, w[slot, 1], 1, 1)

    def gate_up_terms(slot):
        for k, by in enumerate((dg, du)):
            term = dot(a_t[...], by[...])
            count = SIDE * SIDE
            for b in range(count):
                n = width // count
                gu_terms[slot, k, b // SIDE, b % SIDE] = term[b * n : (b + 1) * n].astype(BF16)

    def gu_phases(slot1, slot2, layer, c):
        cols = pl.ds(pl.multiple_of(c * CHUNK, CHUNK), CHUNK)
        return [
            unit_phases(k, k, ring, (send, recv), gu_units[k], gu_terms.at[slot1, k], slot1, slot2, sum_gu.at[layer, k, :, cols]) for k in range(2)
        ]

    def d_phases(c):
        here, last = lax.rem(c, 2), lax.rem(c + 1, 2)
        cols, before = (pl.ds(pl.multiple_of(k * 128, 128), 128) for k in (c, jnp.maximum(c - 1, 0)))
        return [
            unit_phases(2 + k, k, ring, (send, recv), d_units[k], d_terms.at[k, :, :, :, :, cols], here, last, sum_d.at[k, :, :, before]) for k in range(2)
        ]

    def segment(k, phases, condition=None):
        def run():
            for phase in phases:
                phase[k]()

        if condition is None:
            run()
        else:
            pl.when(condition)(run)

    for copy in weights(gu1, 1, 0, 0):
        copy.start()
    prepare(h1, dy)

    @pl.loop(0, chunks)
    def _(c):
        slot, other = lax.rem(c, 2), lax.rem(c + 1, 2)
        for copy in weights(gu1, 1, c, slot):
            copy.wait()

        @pl.when(c < chunks - 1)
        def _():
            for copy in weights(gu1, 1, jnp.minimum(c + 1, chunks - 1), other):
                copy.start()

        @pl.when(c == chunks - 1)
        def _():
            for copy in weights(gu0, 0, 0, other):
                copy.start()

        phases = gu_phases(other, slot, 1, jnp.maximum(c - 2, 0))
        ones, twos = zip(*phases)
        segment(0, ones, c > 0)
        segment(0, twos, c > 1)

        @pl.loop(0, tokens // TILE)
        def _(t):
            tile(t, slot)
            segment(1, twos, (c > 1) & (t == 0))
            segment(1, ones, (c > 0) & (t == 1))

        gate_up_terms(slot)
        down_term(1, c)
        segment(2, ones, c > 0)
        segment(2, twos, c > 1)

    finish()
    prepare(h0, None)

    @pl.loop(0, chunks)
    def _(c):
        copy = pltpu.make_async_copy(p0.at[:, pl.ds(pl.multiple_of(c * CHUNK, CHUNK), CHUNK)], p, load.at[0])
        copy.start()
        copy.wait()
        down_term(0, c)

    first = chunks % 2

    @pl.loop(0, chunks)
    def _(c):
        slot, other = lax.rem(c + first, 2), lax.rem(c + first + 1, 2)
        for copy in weights(gu0, 0, c, slot):
            copy.wait()

        @pl.when(c < chunks - 1)
        def _():
            for copy in weights(gu0, 0, jnp.minimum(c + 1, chunks - 1), other):
                copy.start()

        late = jnp.where(c < 2, 1, 0)
        phases = gu_phases(other, slot, late, lax.rem(c - 2 + chunks, chunks))
        (ones, twos), (d_ones, d_twos) = zip(*phases), zip(*d_phases(c))
        segment(0, ones)
        segment(0, twos)
        segment(0, d_ones)
        segment(0, d_twos, c > 0)

        @pl.loop(0, tokens // TILE)
        def _(t):
            tile(t, slot)
            segment(1, twos, t == 1)
            segment(1, ones, t == 1)
            segment(1, d_ones, t == 3)
            segment(1, d_twos, (t == 3) & (c > 0))

        gate_up_terms(slot)
        segment(2, ones)
        segment(2, twos)
        segment(2, d_ones)
        segment(2, d_twos, c > 0)

    slot, other = (first + chunks) % 2, (first + chunks + 1) % 2
    ones, twos = zip(*gu_phases(other, slot, 0, chunks - 2))
    _, d_twos = zip(*d_phases(jnp.int32(chunks)))
    for k in range(3):
        segment(k, ones)
        segment(k, twos)
        segment(k, d_twos)
        if k == 0:
            finish()
            save = pltpu.make_async_copy(d, dx, load.at[0])
            save.start()
    save.wait()
    _, twos = zip(*gu_phases(slot, other, 0, chunks - 1))
    for k in range(3):
        segment(k, twos)


def backward(h0, h1, dy, p0, gu0, gu1, down, depth, cid):
    tokens, width = h0.shape
    ff = p0.shape[1]
    rows = width // SIDE**2
    blocks = ff // width
    assert blocks * 128 == width and blocks * CHUNK == ff and tokens % TILE == 0
    act = VMEM((tokens, width), BF16)
    scratch = [act, act, VMEM((width, tokens), BF16), act, VMEM((width, tokens), BF16), VMEM((tokens, width), F32)]
    scratch += [VMEM((tokens, CHUNK), BF16)] * 3 + [VMEM((2, 3, width, CHUNK), BF16)]
    scratch += [VMEM((2, 2, SIDE, SIDE, rows, CHUNK), BF16), VMEM((2, SIDE, SIDE, blocks, rows, width), BF16)]
    scratch += [DMA((2,)), DMA((2, 3)), DMA((4, 2, 2, 6)), DMA((4, 2, 2, 6))]
    scratch += unit_scratch((rows,), CHUNK) * 2 + unit_scratch((blocks, rows), 128) * 2
    hbm = pl.BlockSpec(memory_space=pl.ANY)
    vmem = pl.BlockSpec(memory_space=VMEM)
    return pl.pallas_call(
        functools.partial(backward_kernel, depth),
        out_shape=[
            jax.ShapeDtypeStruct((tokens, width), BF16),
            jax.ShapeDtypeStruct((2, 2, rows, ff), F32),
            jax.ShapeDtypeStruct((2, blocks, rows, width), F32),
        ],
        in_specs=[hbm] * 7,
        out_specs=[hbm, vmem, vmem],
        scratch_shapes=scratch,
        compiler_params=pltpu.CompilerParams(collective_id=cid, has_side_effects=True, vmem_limit_bytes=67043328),
        name="backward",
    )(h0, h1, dy, p0, gu0, gu1, down)


def z_scatter_kernel(depth, parts, own, out, in_r, out_r, in_l, out_l, send, recv):
    _, x, y, z, index = place(depth)
    right, left = ({"dp": index(x, y, turn(z, by, depth))} for by in (1, -1))
    meet((right, left))
    copies = Copies(send, recv)
    n_right = depth // 2
    n_left = depth - 1 - n_right
    going = {}
    for s in range(n_right):
        for j in range(parts):
            for way, steps, inbox, outbox, peer in ((1, n_right, in_r, out_r, right), (-1, n_left, in_l, out_l, left)):
                if s >= steps:
                    continue
                value = own[turn(z, way * (steps - s), depth), j]
                if s:
                    going[way, s - 1, j].wait_recv()
                    value += inbox[s - 1, j].astype(F32)
                outbox[s, j] = value.astype(BF16)
                going[way, s, j] = copies.start(outbox.at[s, j], inbox.at[s, j], peer)
    for j in range(parts):
        value = own[z, j]
        for way, steps, inbox in ((1, n_right, in_r), (-1, n_left, in_l)):
            if steps:
                going[way, steps - 1, j].wait_recv()
                value += inbox[steps - 1, j].astype(F32)
        out[j] = value.astype(BF16)
    copies.drain()


def z_scatter(own, cid):
    depth, parts, rows, lanes = own.shape
    boxes = [VMEM((max(steps, 1), parts, rows, lanes), BF16) for steps in (depth // 2, depth // 2, depth - 1 - depth // 2, depth - 1 - depth // 2)]
    count = parts * (depth - 1)
    return pl.pallas_call(
        functools.partial(z_scatter_kernel, depth, parts),
        out_shape=jax.ShapeDtypeStruct(own.shape[1:], BF16),
        in_specs=[pl.BlockSpec(memory_space=VMEM)],
        out_specs=pl.BlockSpec(memory_space=VMEM),
        scratch_shapes=[*boxes, DMA((count,)), DMA((count,))],
        compiler_params=pltpu.CompilerParams(collective_id=cid, has_side_effects=True),
        name="z_scatter",
    )(own)


def flat(t):
    t = t.reshape(-1, 128)
    return jnp.pad(t, ((0, -t.shape[0] % 8), (0, 0)))


def unflat(t, shape):
    size = 1
    for n in shape:
        size *= n
    return t[..., : size // 128, :].reshape(*t.shape[:-2], *shape)


def gather_weights(wg, wu, wd, depth):
    own = jnp.stack([flat(t) for t in (wg[0], wg[1], wd[0], wu[0], wu[1], wd[1])])
    got = z_gather(own, depth, 1)
    g0, g1, d0, u0, u1, d1 = (unflat(got[:, k], t.shape[1:]).reshape(-1, t.shape[2]) for k, t in enumerate((wg, wg, wd, wu, wu, wd)))
    return xy_gather(jnp.stack([g0, u0]), jnp.stack([g1, u1]), jnp.stack([d0, d1]), depth, 2)


def scatter_grads(sums, shapes, depth):
    own = []
    for t, shape in zip(sums, shapes):
        t = t.reshape(depth, -1, 128)
        own.append(jnp.pad(t, ((0, 0), (0, -t.shape[1] % 8), (0, 0))))
    out = z_scatter(jnp.stack(own, 1), 5)
    return [unflat(out[k], shape) for k, shape in enumerate(shapes)]


def solution(mesh):
    n = mesh.shape["dp"]
    depth = n // SIDE**2

    def step(x, dy, wg, wu, wd):
        d_model, ff = wg.shape[1] * n, wg.shape[2]
        gu0, gu1, down = gather_weights(wg, wu, wd, depth)
        gu0, gu1, down = gu0.reshape(2, d_model, ff), gu1.reshape(2, d_model, ff), down.reshape(2, ff, d_model)
        wide = x[0].astype(F32)
        normed = (wide * scale_of(wide)).astype(BF16)
        p0 = (jax.nn.silu(dot(normed, gu0[0])) * dot(normed, gu0[1])).astype(BF16)
        h1 = x[0] + dot(p0, down[0]).astype(BF16)
        dx, sum_gu, sum_d = backward(x[0], h1, dy[0], p0, gu0, gu1, down, depth, 3)
        sums = [*sum_gu[0], sum_d[0], *sum_gu[1], sum_d[1]]
        g0, u0, d0, g1, u1, d1 = scatter_grads(sums, [t.shape[1:] for t in (wg, wu, wd)] * 2, depth)
        return dx[None], jnp.stack([g0, g1]), jnp.stack([u0, u1]), jnp.stack([d0, d1])

    data = P(("rep", "dp"), None, None)
    weight = P(None, "dp", None)
    grad = P("rep", "dp", None)
    return jax.shard_map(step, mesh=mesh, in_specs=(data, data, weight, weight, weight), out_specs=(data, grad, grad, grad), check_vma=False)
```
